32 devices in a mesh: dp: 2 (over z, core), sp: 16 (over x, y).
Axes of the slice: x: 4, y: 4, z: 1, core: 2. Of those that a mesh axis runs over, the one named last changes fastest.
The devices are a block of a 4x4x8 slice.
Arguments:
- q: bfloat16 [64, 48, 128], P('dp'), parts along dimension 0
- k: bfloat16 [64, 8192, 8, 128], P('dp', 'sp'), parts along dimension 0
- v: bfloat16 [64, 8192, 8, 128], P('dp', 'sp'), parts along dimension 0
Outputs:
- q: bfloat16 [64, 48, 128], P('dp'), parts along dimension 0
There are 2 independent parts. The reference program is written for one: setup_inputs(seed, part) draws one part's arguments, and reference() takes and returns one part's arrays. A program takes and returns all parts, laid end to end along the dimension named above; each array names one.
All inputs are finite; a program needn't handle non-finite values.
Results may differ from the reference program's by a relative error of at most 0.012.
Values are sent between devices in bfloat16 or wider.
A program may use at most 768 MiB of HBM per device.

```python
import jax
import jax.numpy as jnp

BATCH = 32
CACHE = 8192
HEADS = 48
KV_HEADS = 8
HEAD = 128


def setup_inputs(seed: int = 0, part: int = 0) -> dict:
    kq, kk, kv = (jax.random.fold_in(k, part) for k in jax.random.split(jax.random.key(seed), 3))
    return {
        "q": (3 * jax.random.normal(kq, (BATCH, HEADS, HEAD), jnp.float32)).astype(jnp.bfloat16),
        "k": jax.random.normal(kk, (BATCH, CACHE, KV_HEADS, HEAD), jnp.float32).astype(jnp.bfloat16),
        "v": jax.random.normal(kv, (BATCH, CACHE, KV_HEADS, HEAD), jnp.float32).astype(jnp.bfloat16),
    }


def einsum(form, a, b):
    return jnp.einsum(form, a.astype(jnp.float32), b.astype(jnp.float32))


def reference(q, k, v):
    grouped = q.reshape(BATCH, KV_HEADS, -1, HEAD)
    scores = einsum("bgsd,bugd->bgsu", grouped, k) * HEAD**-0.5
    weights = jax.nn.softmax(scores, -1).astype(jnp.bfloat16)
    return einsum("bgsu,bugd->bgsd", weights, v).astype(jnp.bfloat16).reshape(BATCH, HEADS, HEAD)
```

```python
import functools

import jax
import jax.numpy as jnp
from jax import lax
from jax.experimental import pallas as pl
from jax.experimental.pallas import tpu as pltpu
from jax.sharding import PartitionSpec as P

MESH = pl.DeviceIdType.MESH
LANES = 128
SUBLANES = 8
TILE = 256
SLOTS = 8
LAG = 6


def kernel(n, heads, q_hbm, k_hbm, v_hbm, out, qs, ks, vs, score_a, score_b, high_a, high_b, part, stat, got, got_stat, q_sem, k_sem, v_sem, part_send, part_recv, stat_send, stat_recv, out_send, out_recv):
    steps, rows, head = q_hbm.shape
    keys = k_hbm.shape[1]
    half = keys // 2
    share = rows // heads
    groups = rows // SUBLANES
    factor = head**-0.5 * 1.4426950408889634
    me = lax.axis_index("sp")

    lane = lax.broadcasted_iota(jnp.int32, (SUBLANES, LANES), 1)
    line = lax.broadcasted_iota(jnp.int32, (SUBLANES, LANES), 0)
    own = [lax.rem(lane, heads) == (line + SUBLANES * r) // share for r in range(groups)]
    wide = [jnp.concatenate([m] * (TILE // LANES), 1) for m in own]
    lane2 = lax.broadcasted_iota(jnp.int32, (2 * SUBLANES, TILE), 1)
    line2 = lax.broadcasted_iota(jnp.int32, (2 * SUBLANES, TILE), 0)
    keep = [jnp.where(lax.rem(lane2, heads) == (line2 + 2 * SUBLANES * r) // share, 1.0, 0.0).astype(jnp.bfloat16) for r in range(groups // 2)]
    low = lane < LANES // 2

    def sequence(s):
        return s // n * n + lax.rem(me + 1 + lax.rem(s, n), n)

    def k_copy(s):
        slot = lax.rem(s, SLOTS)
        return pltpu.make_async_copy(k_hbm.at[sequence(s)], ks.at[slot], k_sem.at[slot])

    def v_copy(s):
        slot = lax.rem(s, SLOTS)
        return pltpu.make_async_copy(v_hbm.at[sequence(s)], vs.at[slot], v_sem.at[slot])

    def part_copy(s):
        turn, j = s // n, lax.rem(s, n)
        owner = lax.rem(me + 1 + j, n)
        return (
            pltpu.make_async_remote_copy(part.at[s], got.at[turn, n - 2 - j], part_send, part_recv.at[turn], device_id={"sp": owner}, device_id_type=MESH),
            pltpu.make_async_remote_copy(stat.at[s], got_stat.at[turn, n - 2 - j], stat_send, stat_recv.at[turn], device_id={"sp": owner}, device_id_type=MESH),
        )

    def scores(s, score, high):
        slot = lax.rem(s, SLOTS)
        q = qs[sequence(s)]
        zero = jnp.zeros_like(q)
        both = jnp.concatenate([jnp.concatenate([q, zero], 1), jnp.concatenate([zero, q], 1)], 0)
        top = jnp.full((SUBLANES, LANES), -jnp.inf, jnp.float32)
        for c in range(half // TILE):
            block = jnp.concatenate([ks[slot, pl.ds(h * half + c * TILE, TILE), :] for h in range(2)], 1)
            all_scores = lax.dot_general(both, block, (((1,), (1,)), ((), ())), preferred_element_type=jnp.float32)
            for h in range(2):
                kept = jnp.full((SUBLANES, TILE), -jnp.inf, jnp.float32)
                for r in range(groups):
                    at = h * rows + r * SUBLANES
                    kept = jnp.where(wide[r], all_scores[at : at + SUBLANES], kept)
                score[h, :, pl.ds(c * TILE, TILE)] = kept
                for i in range(TILE // LANES):
                    top = jnp.maximum(top, kept[:, i * LANES : (i + 1) * LANES])
        high[...] = top

    def values(s, score, high):
        slot = lax.rem(s, SLOTS)
        top = high[...]
        high_row = jnp.zeros_like(top)
        for r in range(groups):
            high_row = jnp.where(own[r], jnp.max(jnp.where(own[r], top, -jnp.inf), 1, keepdims=True), high_row)
        high_wide = jnp.concatenate([high_row] * (TILE // LANES), 1)
        total = jnp.zeros_like(top)
        seen = None
        for c in range(half // TILE):
            weights = []
            for h in range(2):
                w = jnp.exp2((score[h, :, pl.ds(c * TILE, TILE)] - high_wide) * factor)
                for i in range(TILE // LANES):
                    total = total + w[:, i * LANES : (i + 1) * LANES]
                packed = jnp.concatenate([w, w], 0).astype(jnp.bfloat16)
                weights += [packed * m for m in keep]
            block = jnp.concatenate([vs[slot, pl.ds(h * half + c * TILE, TILE), :] for h in range(2)], 1)
            more = jnp.dot(jnp.concatenate(weights, 0), block, preferred_element_type=jnp.float32)
            seen = more if seen is None else seen + more
        total_row = jnp.zeros_like(top)
        for r in range(groups):
            total_row = jnp.where(own[r], jnp.sum(jnp.where(own[r], total, 0.0), 1, keepdims=True), total_row)
        stat[s] = jnp.where(low, high_row, total_row)
        part[s] = (seen[:rows, :head] + seen[rows:, head:]).astype(part.dtype)

    def send(s):
        @pl.when(lax.rem(s, n) != n - 1)
        def _():
            for copy in part_copy(s):
                copy.start()

    def together(turn):
        mine = turn * n + n - 1
        pltpu.make_async_remote_copy(got_stat.at[turn], got_stat.at[turn], stat_send, stat_recv.at[turn], device_id={"sp": me}, device_id_type=MESH).wait_recv()
        stats = [got_stat[turn, p] for p in range(n - 1)] + [stat[mine]]
        top = functools.reduce(jnp.maximum, stats)
        scale = [jnp.exp2((x - top) * factor) for x in stats]
        total = functools.reduce(jnp.add, [x * pltpu.roll(y, LANES // 2, 1) for x, y in zip(scale, stats)])
        scale = [x / total for x in scale]
        pltpu.make_async_remote_copy(got.at[turn], got.at[turn], part_send, part_recv.at[turn], device_id={"sp": me}, device_id_type=MESH).wait_recv()
        result = []
        for r in range(groups):
            first = jnp.logical_and(own[r], lane < heads)
            result.append([jnp.sum(jnp.where(first, x, 0.0), 1, keepdims=True) for x in scale])
        added = None
        for p in range(n):
            x = (got[turn, p] if p < n - 1 else part[mine]).astype(jnp.float32)
            x = x * jnp.concatenate([jnp.broadcast_to(result[r][p], (SUBLANES, head)) for r in range(groups)], 0)
            added = x if added is None else added + x
        at = turn * n + me
        out[at] = added.astype(out.dtype)
        for o in range(1, n):
            pltpu.make_async_remote_copy(out.at[at], out.at[at], out_send, out_recv.at[turn], device_id={"sp": lax.rem(me + o, n)}, device_id_type=MESH).start()

    barrier = pltpu.get_barrier_semaphore()
    pltpu.make_async_copy(q_hbm, qs, q_sem).start()
    for s in range(SLOTS):
        k_copy(s).start()
        v_copy(s).start()
    for o in range(1, n):
        pl.semaphore_signal(barrier, inc=1, device_id={"sp": lax.rem(me + o, n)}, device_id_type=MESH)
    pltpu.make_async_copy(q_hbm, qs, q_sem).wait()
    k_copy(0).wait()
    scores(0, score_a, high_a)
    k_copy(SLOTS).start()
    pl.semaphore_wait(barrier, n - 1)

    def turn_of(s, now, later, last=False):
        v_copy(s).wait()
        if not last:
            k_copy(s + 1).wait()
            scores(s + 1, *later)
        values(s, *now)

        @pl.when(s + SLOTS < steps)
        def _():
            v_copy(s + SLOTS).start()

        @pl.when(s + 1 + SLOTS < steps)
        def _():
            k_copy(s + 1 + SLOTS).start()

    first, second = (score_a, high_a), (score_b, high_b)

    def pair(t, _):
        s = 2 * t

        @pl.when(s > 0)
        def _():
            send(s - 1)

        turn_of(s, first, second)
        send(s)
        turn_of(s + 1, second, first)
        return 0

    at = 0
    for turn in range(steps // n - 1):
        to = ((turn + 1) * n + LAG) // 2
        lax.fori_loop(at, to, pair, 0)
        together(turn)
        at = to
    lax.fori_loop(at, steps // 2 - 1, pair, 0)
    s = steps - 2
    send(s - 1)
    turn_of(s, first, second)
    send(s)
    turn_of(s + 1, second, first, last=True)
    together(steps // n - 1)

    for turn in range(steps // n):
        block = out.at[pl.ds(0, n - 1)]
        pltpu.make_async_remote_copy(block, block, out_send, out_recv.at[turn], device_id={"sp": me}, device_id_type=MESH).wait()
        sent = part.at[pl.ds(0, n - 1)]
        pltpu.make_async_remote_copy(sent, sent, part_send, part_recv.at[turn], device_id={"sp": me}, device_id_type=MESH).wait_send()
        sent = stat.at[pl.ds(0, n - 1)]
        pltpu.make_async_remote_copy(sent, sent, stat_send, stat_recv.at[turn], device_id={"sp": me}, device_id_type=MESH).wait_send()


def attend(n, q, k, v):
    batch, rows, head = q.shape
    heads = k.shape[2]
    keys = k.shape[1] * heads
    turns = batch // n
    flat = (batch, keys, head)
    vmem = pltpu.VMEM
    dma = pltpu.SemaphoreType.DMA
    return pl.pallas_call(
        functools.partial(kernel, n, heads),
        out_shape=jax.ShapeDtypeStruct(q.shape, q.dtype),
        in_specs=[pl.BlockSpec(memory_space=pl.ANY)] * 3,
        out_specs=pl.BlockSpec(memory_space=vmem),
        scratch_shapes=[
            vmem(q.shape, q.dtype),
            vmem((SLOTS, keys, head), k.dtype),
            vmem((SLOTS, keys, head), v.dtype),
            vmem((2, SUBLANES, keys // 2), jnp.float32),
            vmem((2, SUBLANES, keys // 2), jnp.float32),
            vmem((SUBLANES, LANES), jnp.float32),
            vmem((SUBLANES, LANES), jnp.float32),
            vmem((batch, rows, head), q.dtype),
            vmem((batch, SUBLANES, LANES), jnp.float32),
            vmem((turns, n - 1, rows, head), q.dtype),
            vmem((turns, n - 1, SUBLANES, LANES), jnp.float32),
            dma,
            dma((SLOTS,)),
            dma((SLOTS,)),
            dma,
            dma((turns,)),
            dma,
            dma((turns,)),
            dma,
            dma((turns,)),
        ],
        compiler_params=pltpu.CompilerParams(collective_id=0, has_side_effects=True, vmem_limit_bytes=48 * 2**20),
        name="attend",
    )(q, k.reshape(flat), v.reshape(flat))


def solution(mesh):
    n = mesh.shape["sp"]
    return jax.shard_map(
        functools.partial(attend, n),
        mesh=mesh,
        in_specs=(P("dp", None, None), P("dp", "sp", None, None), P("dp", "sp", None, None)),
        out_specs=P("dp", None, None),
        check_vma=False,
    )
```

```python
import functools
import math

import jax
import jax.numpy as jnp
from jax import lax
from jax.experimental import pallas as pl
from jax.experimental.pallas import tpu as pltpu
from jax.sharding import PartitionSpec as P

MESH = pl.DeviceIdType.MESH
LANES = 128
SUBLANES = 8
TILE = 256
DEPTH = 6
GREET = 3
WAIT = 5


def plan(batch, n):
    runs, at = [], 0
    while at < batch:
        owners = 1
        while at + n // owners > batch:
            owners *= 2
        runs.append((at, owners))
        at += n // owners
    return runs


def kernel(n, heads, runs, q_hbm, k_hbm, v_hbm, out, qs, ks, vs, score_a, score_b, high_a, high_b, weight_a, weight_b, part, part_stat, *rest):
    owned, owned_stat = rest[: len(runs)], rest[len(runs) : 2 * len(runs)]
    q_sem, k_sem, v_sem, owned_sent, owned_stat_sent, owned_came, owned_stat_came, out_sent, out_came = rest[2 * len(runs) :]
    batch, rows, head = q_hbm.shape
    pairs = batch // 2
    tail = (batch) // 2
    keys = k_hbm.shape[1]
    half = keys // 2
    share = rows // heads
    groups = rows // SUBLANES
    side = math.isqrt(n)
    factor = head**-0.5 * 1.4426950408889634
    me = lax.axis_index("sp")

    across, along = me // side, lax.rem(me, side)
    hops = [(abs(a - side // 2) + abs(b - side // 2), a, b) for a in range(side) for b in range(side) if a or b]
    others = [lax.rem(across + a, side) * side + lax.rem(along + b, side) for _, a, b in sorted(hops)]

    lane = lax.broadcasted_iota(jnp.int32, (SUBLANES, LANES), 1)
    line = lax.broadcasted_iota(jnp.int32, (SUBLANES, LANES), 0)
    own = [lax.rem(lane, heads) == (line + SUBLANES * r) // share for r in range(groups)]
    wide = [jnp.concatenate([m] * (TILE // LANES), 1) for m in own]
    lane2 = lax.broadcasted_iota(jnp.int32, (2 * SUBLANES, TILE), 1)
    line2 = lax.broadcasted_iota(jnp.int32, (2 * SUBLANES, TILE), 0)
    keep = [jnp.where(lax.rem(lane2, heads) == (line2 + 2 * SUBLANES * r) // share, 1.0, 0.0).astype(jnp.bfloat16) for r in range(groups // 2)]
    low = lane < LANES // 2

    def sequence(s):
        found = s
        for base, owners in reversed(runs):
            count = n // owners
            turned = base + lax.rem(me // owners + 1 + s - base, count)
            found = jnp.where(s < base + count, turned, found)
        return found

    def k_copies(t):
        slot = lax.rem(t, DEPTH)
        return [pltpu.make_async_copy(k_hbm.at[sequence(2 * t + i)], ks.at[slot, i], k_sem.at[slot, i]) for i in range(2)]

    def v_copies(t):
        slot = lax.rem(t, DEPTH)
        return [pltpu.make_async_copy(v_hbm.at[sequence(2 * t + i)], vs.at[slot, i], v_sem.at[slot, i]) for i in range(2)]

    def start(copies):
        for copy in copies:
            copy.start(priority=1)

    def wait(copies):
        for copy in copies:
            copy.wait()

    def scores(t, i, score, high):
        slot = lax.rem(t, DEPTH)
        q = qs[sequence(2 * t + i)]
        zero = jnp.zeros_like(q)
        both = jnp.concatenate([jnp.concatenate([q, zero], 1), jnp.concatenate([zero, q], 1)], 0)
        top = jnp.full((SUBLANES, LANES), -jnp.inf, jnp.float32)
        for c in range(half // TILE):
            block = jnp.concatenate([ks[slot, i, pl.ds(h * half + c * TILE, TILE), :] for h in range(2)], 1)
            all_scores = lax.dot_general(both, block, (((1,), (1,)), ((), ())), preferred_element_type=jnp.float32)
            for h in range(2):
                kept = jnp.full((SUBLANES, TILE), -jnp.inf, jnp.float32)
                for r in range(groups):
                    at = h * rows + r * SUBLANES
                    kept = jnp.where(wide[r], all_scores[at : at + SUBLANES], kept)
                score[h, :, pl.ds(c * TILE, TILE)] = kept
                for l in range(TILE // LANES):
                    top = jnp.maximum(top, kept[:, l * LANES : (l + 1) * LANES])
        high[...] = top

    def weights(t, i, score, high, weight):
        top = high[...]
        high_row = jnp.zeros_like(top)
        for r in range(groups):
            high_row = jnp.where(own[r], jnp.max(jnp.where(own[r], top, -jnp.inf), 1, keepdims=True), high_row)
        high_wide = jnp.concatenate([high_row] * (TILE // LANES), 1)
        total = jnp.zeros_like(top)
        for c in range(half // TILE):
            for h in range(2):
                w = jnp.exp2((score[h, :, pl.ds(c * TILE, TILE)] - high_wide) * factor)
                for l in range(TILE // LANES):
                    total = total + w[:, l * LANES : (l + 1) * LANES]
                packed = jnp.concatenate([w, w], 0).astype(jnp.bfloat16)
                for j, m in enumerate(keep):
                    weight[c, pl.ds(h * rows + 2 * SUBLANES * j, 2 * SUBLANES), :] = packed * m
        total_row = jnp.zeros_like(top)
        for r in range(groups):
            total_row = jnp.where(own[r], jnp.sum(jnp.where(own[r], total, 0.0), 1, keepdims=True), total_row)
        part_stat[2 * t + i] = jnp.where(low, high_row, total_row)

    def values(t, i, weight):
        slot = lax.rem(t, DEPTH)
        seen = None
        for c in range(half // TILE):
            block = jnp.concatenate([vs[slot, i, pl.ds(h * half + c * TILE, TILE), :] for h in range(2)], 1)
            more = jnp.dot(weight[c], block, preferred_element_type=jnp.float32)
            seen = more if seen is None else seen + more
        part[2 * t + i] = (seen[:rows, :head] + seen[rows:, head:]).astype(part.dtype)

    def give(run, q):
        base, owners = runs[run]
        size = rows // owners
        for i in range(owners):
            owner = lax.rem(me // owners + 1 + q - base, n // owners) * owners + i

            @pl.when(owner != me)
            def _():
                slot = lax.rem(me - owner + n, n) - 1
                pltpu.make_async_remote_copy(part.at[q, pl.ds(i * size, size)], owned[run].at[slot], owned_sent.at[run], owned_came.at[run], device_id={"sp": owner}, device_id_type=MESH).start()
                pltpu.make_async_remote_copy(part_stat.at[q], owned_stat[run].at[slot], owned_stat_sent.at[run], owned_stat_came.at[run], device_id={"sp": owner}, device_id_type=MESH).start()

    def together(run):
        base, owners = runs[run]
        size = rows // owners
        mine, place = base + n // owners - 1, base + me // owners
        at = lax.rem(me, owners) * size
        ours = pl.ds(pl.multiple_of(at, SUBLANES), size)
        for block, sem in ((owned_stat[run], owned_stat_came), (owned[run], owned_came)):
            pltpu.make_async_remote_copy(block, block, owned_sent.at[run], sem.at[run], device_id={"sp": me}, device_id_type=MESH).wait_recv()
        stat = [owned_stat[run][p] for p in range(n - 1)] + [part_stat[mine]]
        top = functools.reduce(jnp.maximum, stat)
        scale = [jnp.exp2((x - top) * factor) for x in stat]
        total = functools.reduce(jnp.add, [x * pltpu.roll(y, LANES // 2, 1) for x, y in zip(scale, stat)])
        scale = [x / total for x in scale]
        picks = [lane == (line + SUBLANES * r + at) // share for r in range(size // SUBLANES)]
        added = None
        for p, x in enumerate(scale):
            column = [jnp.broadcast_to(jnp.sum(jnp.where(f, x, 0.0), 1, keepdims=True), (SUBLANES, head)) for f in picks]
            more = (owned[run][p] if p < n - 1 else part[mine, ours]).astype(jnp.float32) * jnp.concatenate(column, 0)
            added = more if added is None else added + more
        out[place, ours] = added.astype(out.dtype)
        block = out.at[place, ours]
        for peer in others:
            pltpu.make_async_remote_copy(block, block, out_sent.at[run], out_came.at[run], device_id={"sp": peer}, device_id_type=MESH).start()

    q_copy = pltpu.make_async_copy(q_hbm, qs, q_sem)
    start(k_copies(0))
    q_copy.start()
    start(k_copies(1))
    for t in range(2, DEPTH):
        start(v_copies(t - 2))
        start(k_copies(t))
    for t in range(DEPTH - 2, DEPTH):
        start(v_copies(t))
    barrier = pltpu.get_barrier_semaphore()
    for o in range(1, n):
        pl.semaphore_signal(barrier, inc=1, device_id={"sp": lax.rem(me + o, n)}, device_id_type=MESH)
    scratch = ((score_a, high_a, weight_a), (score_b, high_b, weight_b))
    wait(k_copies(0))
    q_copy.wait()
    for i in range(2):
        scores(0, i, *scratch[i][:2])
    start(k_copies(DEPTH))
    wait(k_copies(1))
    for i in range(2):
        weights(0, i, *scratch[i])
    for i in range(2):
        scores(1, i, *scratch[i][:2])
    start(k_copies(DEPTH + 1))

    def share_out(t):
        run, t = t if isinstance(t, tuple) else (run_of(t), t)
        for i in range(2):
            give(run, 2 * t + i)

    def run_of(t):
        return max(run for run, (base, _) in enumerate(runs) if base <= 2 * t) if t < tail else None

    def step(run, t, _):
        if run != "nothing":
            share_out((run, t - 1))
        wait(v_copies(t))
        wait(k_copies(t + 2))
        for i in range(2):
            values(t, i, scratch[i][2])
        for i in range(2):
            weights(t + 1, i, *scratch[i])
        for i in range(2):
            scores(t + 2, i, *scratch[i][:2])

        @pl.when(t + DEPTH < pairs)
        def _():
            start(v_copies(t + DEPTH))

        @pl.when(t + 2 + DEPTH < pairs)
        def _():
            start(k_copies(t + 2 + DEPTH))

        return 0

    last = pairs - 1
    lax.fori_loop(0, GREET, functools.partial(step, "nothing"), 0)
    pl.semaphore_wait(barrier, n - 1)
    for t in range(GREET - 1):
        share_out(t)
    bounds = [base // 2 for base, _ in runs[1:]] + [tail]
    events = sorted([(end + 1, 0, run) for run, end in enumerate(bounds)] + [(end + WAIT, 1, run) for run, end in enumerate(bounds)])
    at, now, left = GREET, 0, list(range(len(runs)))
    for stop, kind, run in events:
        if stop < last:
            if stop > at:
                lax.fori_loop(at, stop, functools.partial(step, now), 0)
                at = stop
            if kind == 0:
                now = run + 1 if run + 1 < len(runs) else None
            else:
                together(run)
                left.remove(run)
    lax.fori_loop(at, last - 1, functools.partial(step, now), 0)
    share_out(last - 2)
    wait(v_copies(last - 1))
    for i in range(2):
        values(last - 1, i, scratch[i][2])
    for i in range(2):
        weights(last, i, *scratch[i])
    share_out(last - 1)
    for i in range(2):
        v_copies(last)[i].wait()
        values(last, i, scratch[i][2])
        give(run_of(last), 2 * last + i)
    for run in left:
        together(run)

    for run, (base, owners) in enumerate(runs):
        block = out.at[pl.ds(0, n - 1), pl.ds(0, rows // owners)]
        pltpu.make_async_remote_copy(block, block, out_sent.at[run], out_came.at[run], device_id={"sp": me}, device_id_type=MESH).wait()
        for block, sem in ((owned[run], owned_sent), (owned_stat[run], owned_stat_sent)):
            pltpu.make_async_remote_copy(block, block, sem.at[run], owned_came.at[run], device_id={"sp": me}, device_id_type=MESH).wait_send()


def attend(n, q, k, v):
    batch, rows, head = q.shape
    heads = k.shape[2]
    keys = k.shape[1] * heads
    runs = plan(batch, n)
    flat = (batch, keys, head)
    vmem = pltpu.VMEM
    dma = pltpu.SemaphoreType.DMA
    return pl.pallas_call(
        functools.partial(kernel, n, heads, runs),
        out_shape=jax.ShapeDtypeStruct(q.shape, q.dtype),
        in_specs=[pl.BlockSpec(memory_space=pltpu.HBM)] * 3,
        out_specs=pl.BlockSpec(memory_space=vmem),
        scratch_shapes=[
            vmem(q.shape, q.dtype),
            vmem((DEPTH, 2, keys, head), k.dtype),
            vmem((DEPTH, 2, keys, head), v.dtype),
            vmem((2, SUBLANES, keys // 2), jnp.float32),
            vmem((2, SUBLANES, keys // 2), jnp.float32),
            vmem((SUBLANES, LANES), jnp.float32),
            vmem((SUBLANES, LANES), jnp.float32),
            vmem((keys // 2 // TILE, 2 * rows, TILE), q.dtype),
            vmem((keys // 2 // TILE, 2 * rows, TILE), q.dtype),
            vmem((batch, rows, head), q.dtype),
            vmem((batch, SUBLANES, LANES), jnp.float32),
            *[vmem((n - 1, rows // owners, head), q.dtype) for _, owners in runs],
            *[vmem((n - 1, SUBLANES, LANES), jnp.float32) for _ in runs],
            dma,
            dma((DEPTH, 2)),
            dma((DEPTH, 2)),
            *[dma((len(runs),))] * 6,
        ],
        compiler_params=pltpu.CompilerParams(collective_id=0, has_side_effects=True, vmem_limit_bytes=52 * 2**20),
        name="attend",
    )(pltpu.with_memory_space_constraint(q, pltpu.HBM), k.reshape(flat), v.reshape(flat))


def solution(mesh):
    n = mesh.shape["sp"]
    return jax.shard_map(
        functools.partial(attend, n),
        mesh=mesh,
        in_specs=(P("dp", None, None), P("dp", "sp", None, None), P("dp", "sp", None, None)),
        out_specs=P("dp", None, None),
        check_vma=False,
    )
```

```python
import functools
import math

import jax
import jax.numpy as jnp
from jax import lax
from jax.experimental import pallas as pl
from jax.experimental.pallas import tpu as pltpu
from jax.sharding import PartitionSpec as P

MESH = pl.DeviceIdType.MESH
LANES = 128
SUBLANES = 8
TILE = 256
DEPTH = 6
GREET = 2
WAIT = 100


def plan(batch, n):
    runs, at = [], 0
    while at < batch:
        owners = 1
        while at + n // owners > batch:
            owners *= 2
        runs.append((at, owners))
        at += n // owners
    return runs


def kernel(n, heads, runs, q_hbm, k_hbm, v_hbm, out, qs, ks, vs, score_a, score_b, high_a, high_b, weight_a, weight_b, part, part_stat, *rest):
    owned, owned_stat = rest[: len(runs)], rest[len(runs) : 2 * len(runs)]
    q_sem, k_sem, v_sem, owned_sent, owned_stat_sent, owned_came, owned_stat_came, out_sent, out_came = rest[2 * len(runs) :]
    batch, rows, head = q_hbm.shape
    pairs = batch // 2
    tail = (batch) // 2
    keys = k_hbm.shape[1]
    half = keys // 2
    share = rows // heads
    groups = rows // SUBLANES
    side = math.isqrt(n)
    factor = head**-0.5 * 1.4426950408889634
    me = lax.axis_index("sp")

    across, along = me // side, lax.rem(me, side)
    hops = [(abs(a - side // 2) + abs(b - side // 2), a, b) for a in range(side) for b in range(side) if a or b]
    others = [lax.rem(across + a, side) * side + lax.rem(along + b, side) for _, a, b in sorted(hops)]

    lane = lax.broadcasted_iota(jnp.int32, (SUBLANES, LANES), 1)
    line = lax.broadcasted_iota(jnp.int32, (SUBLANES, LANES), 0)
    own = [lax.rem(lane, heads) == (line + SUBLANES * r) // share for r in range(groups)]
    wide = [jnp.concatenate([m] * (TILE // LANES), 1) for m in own]
    lane2 = lax.broadcasted_iota(jnp.int32, (2 * SUBLANES, TILE), 1)
    line2 = lax.broadcasted_iota(jnp.int32, (2 * SUBLANES, TILE), 0)
    keep = [jnp.where(lax.rem(lane2, heads) == (line2 + 2 * SUBLANES * r) // share, 1.0, 0.0).astype(jnp.bfloat16) for r in range(groups // 2)]
    low = lane < LANES // 2

    def sequence(s):
        found = s
        for base, owners in reversed(runs):
            count = n // owners
            turned = base + lax.rem(me // owners + 1 + s - base, count)
            found = jnp.where(s < base + count, turned, found)
        return found

    def k_copies(t):
        slot = lax.rem(t, DEPTH)
        return [pltpu.make_async_copy(k_hbm.at[sequence(2 * t + i)], ks.at[slot, i], k_sem.at[slot, i]) for i in range(2)]

    def v_copies(t):
        slot = lax.rem(t, DEPTH)
        return [pltpu.make_async_copy(v_hbm.at[sequence(2 * t + i)], vs.at[slot, i], v_sem.at[slot, i]) for i in range(2)]

    def start(copies):
        for copy in copies:
            copy.start(priority=1)

    def wait(copies):
        for copy in copies:
            copy.wait()

    def scores(t, i, score, high):
        slot = lax.rem(t, DEPTH)
        q = qs[sequence(2 * t + i)]
        zero = jnp.zeros_like(q)
        both = jnp.concatenate([jnp.concatenate([q, zero], 1), jnp.concatenate([zero, q], 1)], 0)
        top = jnp.full((SUBLANES, LANES), -jnp.inf, jnp.float32)
        for c in range(half // TILE):
            block = jnp.concatenate([ks[slot, i, pl.ds(h * half + c * TILE, TILE), :] for h in range(2)], 1)
            all_scores = lax.dot_general(both, block, (((1,), (1,)), ((), ())), preferred_element_type=jnp.float32)
            for h in range(2):
                kept = jnp.full((SUBLANES, TILE), -jnp.inf, jnp.float32)
                for r in range(groups):
                    at = h * rows + r * SUBLANES
                    kept = jnp.where(wide[r], all_scores[at : at + SUBLANES], kept)
                score[h, :, pl.ds(c * TILE, TILE)] = kept
                for l in range(TILE // LANES):
                    top = jnp.maximum(top, kept[:, l * LANES : (l + 1) * LANES])
        high[...] = top

    def weights(t, i, score, high, weight):
        top = high[...]
        high_row = jnp.zeros_like(top)
        for r in range(groups):
            high_row = jnp.where(own[r], jnp.max(jnp.where(own[r], top, -jnp.inf), 1, keepdims=True), high_row)
        high_wide = jnp.concatenate([high_row] * (TILE // LANES), 1)
        total = jnp.zeros_like(top)
        for c in range(half // TILE):
            for h in range(2):
                w = jnp.exp2((score[h, :, pl.ds(c * TILE, TILE)] - high_wide) * factor)
                for l in range(TILE // LANES):
                    total = total + w[:, l * LANES : (l + 1) * LANES]
                packed = jnp.concatenate([w, w], 0).astype(jnp.bfloat16)
                for j, m in enumerate(keep):
                    weight[c, pl.ds(h * rows + 2 * SUBLANES * j, 2 * SUBLANES), :] = packed * m
        total_row = jnp.zeros_like(top)
        for r in range(groups):
            total_row = jnp.where(own[r], jnp.sum(jnp.where(own[r], total, 0.0), 1, keepdims=True), total_row)
        part_stat[2 * t + i] = jnp.where(low, high_row, total_row)

    def values(t, i, weight):
        slot = lax.rem(t, DEPTH)
        seen = None
        for c in range(half // TILE):
            block = jnp.concatenate([vs[slot, i, pl.ds(h * half + c * TILE, TILE), :] for h in range(2)], 1)
            more = jnp.dot(weight[c], block, preferred_element_type=jnp.float32)
            seen = more if seen is None else seen + more
        part[2 * t + i] = (seen[:rows, :head] + seen[rows:, head:]).astype(part.dtype)

    def give(run, q, stats=True, values=True):
        base, owners = runs[run]
        size = rows // owners
        for i in range(owners):
            owner = lax.rem(me // owners + 1 + q - base, n // owners) * owners + i

            @pl.when(owner != me)
            def _():
                slot = lax.rem(me - owner + n, n) - 1
                if stats:
                    pltpu.make_async_remote_copy(part_stat.at[q], owned_stat[run].at[slot], owned_stat_sent.at[run], owned_stat_came.at[run], device_id={"sp": owner}, device_id_type=MESH).start()
                if values:
                    pltpu.make_async_remote_copy(part.at[q, pl.ds(i * size, size)], owned[run].at[slot], owned_sent.at[run], owned_came.at[run], device_id={"sp": owner}, device_id_type=MESH).start()

    def together(run):
        base, owners = runs[run]
        size = rows // owners
        mine, place = base + n // owners - 1, base + me // owners
        at = lax.rem(me, owners) * size
        ours = pl.ds(pl.multiple_of(at, SUBLANES), size)
        block = owned_stat[run]
        pltpu.make_async_remote_copy(block, block, owned_sent.at[run], owned_stat_came.at[run], device_id={"sp": me}, device_id_type=MESH).wait_recv()
        stat = [owned_stat[run][p] for p in range(n - 1)] + [part_stat[mine]]
        top = functools.reduce(jnp.maximum, stat)
        scale = [jnp.exp2((x - top) * factor) for x in stat]
        total = functools.reduce(jnp.add, [x * pltpu.roll(y, LANES // 2, 1) for x, y in zip(scale, stat)])
        scale = [x / total for x in scale]
        picks = [lane == (line + SUBLANES * r + at) // share for r in range(size // SUBLANES)]
        columns = [[jnp.broadcast_to(jnp.sum(jnp.where(f, x, 0.0), 1, keepdims=True), (SUBLANES, head)) for f in picks] for x in scale]
        block = owned[run]
        pltpu.make_async_remote_copy(block, block, owned_sent.at[run], owned_came.at[run], device_id={"sp": me}, device_id_type=MESH).wait_recv()
        added = None
        for p, column in enumerate(columns):
            more = (owned[run][p] if p < n - 1 else part[mine, ours]).astype(jnp.float32) * jnp.concatenate(column, 0)
            added = more if added is None else added + more
        out[place, ours] = added.astype(out.dtype)
        block = out.at[place, ours]
        for peer in others:
            pltpu.make_async_remote_copy(block, block, out_sent.at[run], out_came.at[run], device_id={"sp": peer}, device_id_type=MESH).start()

    q_copy = pltpu.make_async_copy(q_hbm, qs, q_sem)
    start(k_copies(0))
    q_copy.start()
    start(k_copies(1))
    for t in range(2, DEPTH):
        start(v_copies(t - 2))
        start(k_copies(t))
    for t in range(DEPTH - 2, DEPTH):
        start(v_copies(t))
    barrier = pltpu.get_barrier_semaphore()
    for o in range(1, n):
        pl.semaphore_signal(barrier, inc=1, device_id={"sp": lax.rem(me + o, n)}, device_id_type=MESH)
    scratch = ((score_a, high_a, weight_a), (score_b, high_b, weight_b))
    wait(k_copies(0))
    q_copy.wait()
    for i in range(2):
        scores(0, i, *scratch[i][:2])
    start(k_copies(DEPTH))
    wait(k_copies(1))
    for i in range(2):
        weights(0, i, *scratch[i])
    for i in range(2):
        scores(1, i, *scratch[i][:2])
    start(k_copies(DEPTH + 1))

    def share_out(t):
        run, t = t if isinstance(t, tuple) else (run_of(t), t)
        for i in range(2):
            give(run, 2 * t + i)

    def run_of(t):
        return max(run for run, (base, _) in enumerate(runs) if base <= 2 * t) if t < tail else None

    def step(run, t, _):
        if run != "nothing":
            share_out((run, t - 1))
        wait(v_copies(t))
        wait(k_copies(t + 2))
        for i in range(2):
            values(t, i, scratch[i][2])
        for i in range(2):
            weights(t + 1, i, *scratch[i])
        for i in range(2):
            scores(t + 2, i, *scratch[i][:2])

        @pl.when(t + DEPTH < pairs)
        def _():
            start(v_copies(t + DEPTH))

        @pl.when(t + 2 + DEPTH < pairs)
        def _():
            start(k_copies(t + 2 + DEPTH))

        return 0

    last = pairs - 1
    lax.fori_loop(0, GREET, functools.partial(step, "nothing"), 0)
    pl.semaphore_wait(barrier, n - 1)
    for t in range(GREET - 1):
        share_out(t)
    bounds = [base // 2 for base, _ in runs[1:]] + [tail]
    events = sorted([(end + 1, 0, run) for run, end in enumerate(bounds)] + [(end + WAIT, 1, run) for run, end in enumerate(bounds)])
    at, now, left = GREET, 0, list(range(len(runs)))
    for stop, kind, run in events:
        if stop < last:
            if stop > at:
                lax.fori_loop(at, stop, functools.partial(step, now), 0)
                at = stop
            if kind == 0:
                now = run + 1 if run + 1 < len(runs) else None
            else:
                together(run)
                left.remove(run)
    lax.fori_loop(at, last - 1, functools.partial(step, now), 0)
    share_out(last - 2)
    wait(v_copies(last - 1))
    for i in range(2):
        values(last - 1, i, scratch[i][2])
    for i in range(2):
        weights(last, i, *scratch[i])
    share_out(last - 1)
    for i in range(2):
        give(run_of(last), 2 * last + i, values=False)
    for i in range(2):
        v_copies(last)[i].wait()
        values(last, i, scratch[i][2])
        give(run_of(last), 2 * last + i, stats=False)
    for run in left:
        together(run)

    for run, (base, owners) in enumerate(runs):
        block = out.at[pl.ds(0, n - 1), pl.ds(0, rows // owners)]
        pltpu.make_async_remote_copy(block, block, out_sent.at[run], out_came.at[run], device_id={"sp": me}, device_id_type=MESH).wait()
        for block, sem in ((owned[run], owned_sent), (owned_stat[run], owned_stat_sent)):
            pltpu.make_async_remote_copy(block, block, sem.at[run], owned_came.at[run], device_id={"sp": me}, device_id_type=MESH).wait_send()


def attend(n, q, k, v):
    batch, rows, head = q.shape
    heads = k.shape[2]
    keys = k.shape[1] * heads
    runs = plan(batch, n)
    flat = (batch, keys, head)
    vmem = pltpu.VMEM
    dma = pltpu.SemaphoreType.DMA
    return pl.pallas_call(
        functools.partial(kernel, n, heads, runs),
        out_shape=jax.ShapeDtypeStruct(q.shape, q.dtype),
        in_specs=[pl.BlockSpec(memory_space=pltpu.HBM)] * 3,
        out_specs=pl.BlockSpec(memory_space=vmem),
        scratch_shapes=[
            vmem(q.shape, q.dtype),
            vmem((DEPTH, 2, keys, head), k.dtype),
            vmem((DEPTH, 2, keys, head), v.dtype),
            vmem((2, SUBLANES, keys // 2), jnp.float32),
            vmem((2, SUBLANES, keys // 2), jnp.float32),
            vmem((SUBLANES, LANES), jnp.float32),
            vmem((SUBLANES, LANES), jnp.float32),
            vmem((keys // 2 // TILE, 2 * rows, TILE), q.dtype),
            vmem((keys // 2 // TILE, 2 * rows, TILE), q.dtype),
            vmem((batch, rows, head), q.dtype),
            vmem((batch, SUBLANES, LANES), jnp.float32),
            *[vmem((n - 1, rows // owners, head), q.dtype) for _, owners in runs],
            *[vmem((n - 1, SUBLANES, LANES), jnp.float32) for _ in runs],
            dma,
            dma((DEPTH, 2)),
            dma((DEPTH, 2)),
            *[dma((len(runs),))] * 6,
        ],
        compiler_params=pltpu.CompilerParams(collective_id=0, has_side_effects=True, vmem_limit_bytes=52 * 2**20),
        name="attend",
    )(pltpu.with_memory_space_constraint(q, pltpu.HBM), k.reshape(flat), v.reshape(flat))


def solution(mesh):
    n = mesh.shape["sp"]
    return jax.shard_map(
        functools.partial(attend, n),
        mesh=mesh,
        in_specs=(P("dp", None, None), P("dp", "sp", None, None), P("dp", "sp", None, None)),
        out_specs=P("dp", None, None),
        check_vma=False,
    )
```
